32 devices in a mesh: dp: 2 (over x), fsdp: 16 (over z, y, core).
Axes of the slice: x: 2, y: 2, z: 4, core: 2. Of those that a mesh axis runs over, the one named last changes fastest.
Arguments:
- byte_ids: int32 [2, 2048], P('dp', 'fsdp'), may hold values from 0 to 255
- cotangent: bfloat16 [2, 2048, 1024], P('dp', 'fsdp'), may hold values from -6 to 6
- patch_table: bfloat16 [2048, 128], P('fsdp'), may hold values from -6 to 6
- global_gain: bfloat16 [1024], P('fsdp'), may hold values from 0.099609375 to 1.8984375
- in_proj: bfloat16 [1024, 4384], P('fsdp'), may hold values from -0.1875 to 0.1875
- conv_weight: bfloat16 [2304, 4], P('fsdp'), may hold values from -3 to 3
- conv_bias: bfloat16 [2304], P('fsdp'), may hold values from -0.5 to 0.5
- step_bias: bfloat16 [32], P('fsdp'), may hold values from -7 to -3
- decay_log: bfloat16 [32], P('fsdp'), may hold values from -1 to 1
- skip_gain: bfloat16 [32], P('fsdp'), may hold values from 0.5 to 1.5
- mixer_gain: bfloat16 [2048], P('fsdp'), may hold values from 0.099609375 to 1.8984375
- out_proj: bfloat16 [2048, 1024], P('fsdp'), may hold values from -0.125 to 0.125
- byte_table: bfloat16 [256, 1024], P('fsdp'), may hold values from -6 to 6
- local_gain: bfloat16 [1024], P('fsdp'), may hold values from 0.099609375 to 1.8984375
- qkv_proj: bfloat16 [1024, 3072], P('fsdp'), may hold values from -0.1875 to 0.1875
- attn_out: bfloat16 [1024, 1024], P('fsdp'), may hold values from -0.375 to 0.375
- ffn_gain: bfloat16 [1024], P('fsdp'), may hold values from 0.099609375 to 1.8984375
- gate_up: bfloat16 [1024, 8192], P('fsdp'), may hold values from -0.1875 to 0.1875
- down_proj: bfloat16 [4096, 1024], P('fsdp'), may hold values from -0.125 to 0.125
Outputs:
- activations: bfloat16 [2, 2048, 1024], P('dp', 'fsdp')
- patch_table_grad: float32 [2048, 128], P('fsdp')
- global_gain_grad: float32 [1024], P('fsdp')
- in_proj_grad: float32 [1024, 4384], P('fsdp')
- conv_weight_grad: float32 [2304, 4], P('fsdp')
- conv_bias_grad: float32 [2304], P('fsdp')
- step_bias_grad: float32 [32], P('fsdp')
- decay_log_grad: float32 [32], P('fsdp')
- skip_gain_grad: float32 [32], P('fsdp')
- mixer_gain_grad: float32 [2048], P('fsdp')
- out_proj_grad: float32 [2048, 1024], P('fsdp')
- byte_table_grad: float32 [256, 1024], P('fsdp')
- local_gain_grad: float32 [1024], P('fsdp')
- qkv_proj_grad: float32 [1024, 3072], P('fsdp')
- attn_out_grad: float32 [1024, 1024], P('fsdp')
- ffn_gain_grad: float32 [1024], P('fsdp')
- gate_up_grad: float32 [1024, 8192], P('fsdp')
- down_proj_grad: float32 [4096, 1024], P('fsdp')
The draws below stay inside these ranges and needn't reach their ends.
All inputs are finite; a program needn't handle non-finite values.
Results may differ from the reference program's by a relative error of at most 0.03.
Values may be sent and summed in bfloat16 or wider, within the bound.
A program may use at most 320 MiB of HBM per device.

```python
import math
import jax
import jax.numpy as jnp
import numpy as np
from jax import lax

D = 1024
NST = 128
HM = 32
HA = 16
FF = 4096
VOCAB = 256
KC = 4
PATCH = 8
TOK_DEV = 128
DI = 2048
PM = 64
DA = 64
DG = 128
XBC = 2304
INW = 4384
LENGTH = 2048
BATCH = 2


def with_ends(values, own_key, smallest, top_value):
    longest = values.shape.index(max(values.shape))
    spots = []
    for shift in (0, 1):
        where = [jax.random.randint(jax.random.fold_in(own_key, axis), (), 0, length) for axis, length in enumerate(values.shape)]
        where[longest] = (where[longest] + shift) % values.shape[longest]
        spots.append(tuple(where))
    return values.at[spots[0]].set(smallest).at[spots[1]].set(top_value)


def steps_of(rng, dims, cuts, least, largest):
    level = 1.0
    for dim, blocks in cuts:
        steps = jax.random.uniform(jax.random.fold_in(jax.random.fold_in(rng, 6), dim), (blocks,), jnp.float32, least / len(cuts), largest / len(cuts))
        level = level * jnp.repeat(jnp.exp(steps), dims[dim] // blocks).reshape((-1,) + (1,) * (len(dims) - 1 - dim))
    return level


def rank_bounds(count, lean):
    weights = [(1 << 20) // math.isqrt(rank ** lean) + 1 for rank in range(1, count + 1)]
    deviation = 1 + sum(weights) // (1 << 30)
    return np.cumsum(np.array([max(1, weight // deviation) for weight in weights]))


def ranked_ids(key, dims, amount, slope):
    grid = rank_bounds(amount, slope)
    ticket = jax.random.randint(jax.random.fold_in(key, 1), dims, 0, int(grid[amount - 1]))
    grade = jnp.searchsorted(jnp.asarray(grid, jnp.int32), ticket, side="right")
    return jax.random.permutation(jax.random.fold_in(key, 2), amount)[grade].astype(jnp.int32)


def normal_values(rng, shape, deviation, most, split=(), held_as=jnp.bfloat16):
    array = jax.random.normal(rng, shape, jnp.float32) * deviation
    if len(split) > 0:
        array = steps_of(rng, shape, split, -0.22, 0.18) * array
    return jnp.clip(array, min=-most, max=most).astype(held_as)


def setup_inputs(seed: int = 0) -> dict:
    key_list = jax.random.split(jax.random.key(seed), 20)
    byte_ids = with_ends(ranked_ids(key_list[0], (BATCH, LENGTH), VOCAB, 1), jax.random.fold_in(key_list[0], 3), 0, VOCAB - 1).astype(jnp.int32)
    cotangent = normal_values(key_list[1], (BATCH, LENGTH, D), 1.0, 6.0, ((0, 2), (1, 16)))
    patch_table = normal_values(key_list[2], (PATCH * VOCAB, DG), 1.0, 6.0, ((0, 16),))
    global_gain = jnp.clip(1.0 + 0.18 * jax.random.normal(key_list[3], (D,), jnp.float32), 0.099609375, 1.8984375).astype(jnp.bfloat16)
    in_proj = normal_values(key_list[4], (D, INW), D ** -0.5, 0.1875, ((0, 16),))
    conv_weight = normal_values(key_list[5], (XBC, KC), KC ** -0.5, 3.0, ((0, 16),))
    conv_bias = jnp.clip(jax.random.uniform(key_list[6], (XBC,), jnp.float32, -0.5, 0.5) * steps_of(key_list[6], (XBC,), ((0, 16),), -0.4, 0.0), -0.5, 0.5).astype(jnp.bfloat16)
    step_bias = jnp.clip(-7.0 + 4.0 * jax.random.uniform(key_list[7], (HM,), jnp.float32) ** steps_of(key_list[7], (HM,), ((0, 16),), -0.2, 0.2), -7.0, -3.0).astype(jnp.bfloat16)
    decay_log = jnp.clip(jax.random.uniform(key_list[8], (HM,), jnp.float32, -1.0, 1.0) * steps_of(key_list[8], (HM,), ((0, 16),), -0.4, 0.0), -1.0, 1.0).astype(jnp.bfloat16)
    skip_gain = jnp.clip(0.5 + 1.0 * jax.random.uniform(key_list[9], (HM,), jnp.float32) ** steps_of(key_list[9], (HM,), ((0, 16),), -0.2, 0.2), 0.5, 1.5).astype(jnp.bfloat16)
    mixer_gain = jnp.clip(1.0 + 0.18 * jax.random.normal(key_list[10], (DI,), jnp.float32), 0.099609375, 1.8984375).astype(jnp.bfloat16)
    out_proj = normal_values(key_list[11], (DI, D), DI ** -0.5, 0.125, ((0, 16),))
    byte_table = normal_values(key_list[12], (VOCAB, D), 1.0, 6.0, ((0, 16),))
    local_gain = jnp.clip(1.0 + 0.18 * jax.random.normal(key_list[13], (D,), jnp.float32), 0.099609375, 1.8984375).astype(jnp.bfloat16)
    qkv_proj = normal_values(key_list[14], (D, 3 * D), D ** -0.5, 0.1875, ((0, 16),))
    attn_out = normal_values(key_list[15], (D, D), (D // 4) ** -0.5, 0.375, ((0, 16),))
    ffn_gain = jnp.clip(1.0 + 0.18 * jax.random.normal(key_list[16], (D,), jnp.float32), 0.099609375, 1.8984375).astype(jnp.bfloat16)
    gate_up = normal_values(key_list[17], (D, 2 * FF), D ** -0.5, 0.1875, ((0, 16),))
    down_proj = normal_values(key_list[18], (FF, D), (FF // 2) ** -0.5, 0.125, ((0, 16),))
    return {"byte_ids": byte_ids, "cotangent": cotangent, "patch_table": patch_table, "global_gain": global_gain, "in_proj": in_proj, "conv_weight": conv_weight, "conv_bias": conv_bias, "step_bias": step_bias, "decay_log": decay_log, "skip_gain": skip_gain, "mixer_gain": mixer_gain, "out_proj": out_proj, "byte_table": byte_table, "local_gain": local_gain, "qkv_proj": qkv_proj, "attn_out": attn_out, "ffn_gain": ffn_gain, "gate_up": gate_up, "down_proj": down_proj}


highest = lax.Precision.HIGHEST
epsilon = 1e-05

@jax.custom_vjp
def low(v):
    return lax.optimization_barrier(v.astype(jnp.bfloat16)).astype(jnp.float32)

@jax.custom_vjp
def low_back(v):
    return v

def low_keep(v):
    return (low(v), None)

def low_pass(kept, grad):
    return (grad,)

def back_keep(v):
    return (v, None)

def back_low(kept, grad):
    return (low(grad),)
low.defvjp(low_keep, low_pass)
low_back.defvjp(back_keep, back_low)

def scale_rows(values, scale_gain):
    return values * lax.rsqrt(lax.optimization_barrier(jnp.mean(values * values, axis=-1, keepdims=True)) + epsilon) * scale_gain

def project(values, matrix):
    return low_back(jnp.dot(low(values), matrix, precision=highest, preferred_element_type=jnp.float32))

def state_blocks(inputs, b_rows, c_rows, step_size, decay_rate, skip_gain):
    cumulative = jnp.cumsum(step_size * decay_rate, axis=1)
    length = inputs.shape[1]
    causal = (jnp.arange(length)[None, :] <= jnp.arange(length)[:, None])[None, :, :, None]
    spread = cumulative[:, :, None, :] - cumulative[:, None, :, :]
    weights = jnp.exp(jnp.where(causal, spread, -jnp.inf))
    intersection = jnp.einsum('btn,bun->btu', c_rows, b_rows, precision=highest)
    scaled = inputs * step_size[..., None]
    local_out = jnp.einsum('btuh,buhp->bthp', intersection[..., None] * weights, scaled, precision=highest)
    local_out = local_out + skip_gain[:, None] * inputs
    tail_decay = jnp.exp(cumulative[:, -1:, :] - cumulative)
    summary = jnp.einsum('buh,buhp,bun->bhpn', tail_decay, scaled, b_rows, precision=highest)
    return (local_out, cumulative, summary, jnp.exp(cumulative[:, -1, :]))

def state_join(local_out, c_rows, cumulative, state_in):
    carried = jnp.einsum('btn,bhpn->bthp', c_rows, state_in, precision=highest)
    return local_out + carried * jnp.exp(cumulative)[..., None]

def patch_attention(qkv_rows):
    patches = qkv_rows.shape[0] // PATCH
    pieces = qkv_rows.reshape(patches, PATCH, 3, HA, DA)
    scores = jnp.einsum('pihd,pjhd->phij', pieces[:, :, 0], pieces[:, :, 1], precision=highest) * DA ** (-0.5)
    causal = jnp.arange(PATCH)[None, :] <= jnp.arange(PATCH)[:, None]
    scores = jnp.where(causal, scores, -1e+30)
    attention_weights = jax.nn.softmax(scores, axis=-1)
    combined = jnp.einsum('phij,pjhd->pihd', attention_weights, pieces[:, :, 2], precision=highest)
    return combined.reshape(patches * PATCH, HA * DA)

def layer(params, sequence):
    patch_table, global_gain, in_proj, conv_weight, conv_bias, step_bias, decay_log, skip_gain, mixer_gain, out_proj, byte_table, local_gain, qkv_proj, attn_out, ffn_gain, gate_up, down_proj = params
    patches = sequence.shape[0] // PATCH
    patch_grid = sequence.reshape(patches, PATCH)
    earlier = jnp.concatenate([jnp.zeros((1, PATCH), jnp.int32), patch_grid[:-1]], 0)
    lookup = earlier + VOCAB * jnp.arange(PATCH, dtype=jnp.int32)[None, :]
    keep_row = (jnp.arange(patches) > 0).astype(jnp.float32)[:, None]
    patch_input = low_back(patch_table[lookup].reshape(patches, D) * keep_row)
    projected = project(scale_rows(patch_input, global_gain), in_proj)
    gate_z = projected[:, :DI]
    conv_input = projected[:, DI:DI + XBC]
    step_raw = projected[:, DI + XBC:]
    padded = jnp.concatenate([jnp.zeros((KC - 1, XBC), jnp.float32), conv_input], 0)
    summed = conv_bias
    for offset in range(KC):
        summed = summed + padded[offset:offset + patches] * conv_weight[:, offset]
    conv_out = jax.nn.silu(summed)
    block_size = TOK_DEV // PATCH
    block_count = patches // block_size
    inputs = conv_out[:, :DI].reshape(block_count, block_size, HM, PM)
    b_rows = conv_out[:, DI:DI + NST].reshape(block_count, block_size, NST)
    c_rows = conv_out[:, DI + NST:].reshape(block_count, block_size, NST)
    step_size = jax.nn.softplus(step_raw + step_bias).reshape(block_count, block_size, HM)
    local_out, cumulative, summary, decay_total = state_blocks(inputs, b_rows, c_rows, step_size, -jnp.exp(decay_log), skip_gain)

    def carry_state(carried, element):
        return (element[0][:, None, None] * carried + element[1], carried)
    _, state_in = lax.scan(carry_state, jnp.zeros((HM, PM, NST), jnp.float32), (decay_total, summary))
    joined = state_join(local_out, c_rows, cumulative, state_in).reshape(patches, DI)
    mixer_norm = scale_rows(joined * jax.nn.silu(gate_z), mixer_gain)
    patch_out = patch_input + project(mixer_norm, out_proj)
    stream = low_back(byte_table[sequence]) + jnp.repeat(patch_out, PATCH, axis=0)
    qkv_rows = project(scale_rows(stream, local_gain), qkv_proj)
    residual = stream + project(patch_attention(qkv_rows), attn_out)
    gate_vals = project(scale_rows(residual, ffn_gain), gate_up)
    hidden = jax.nn.silu(gate_vals[:, :FF]) * gate_vals[:, FF:]
    return residual + project(hidden, down_proj)

def reference(byte_ids, cotangent, patch_table, global_gain, in_proj, conv_weight, conv_bias, step_bias, decay_log, skip_gain, mixer_gain, out_proj, byte_table, local_gain, qkv_proj, attn_out, ffn_gain, gate_up, down_proj):
    params = tuple((matrix.astype(jnp.float32) for matrix in (patch_table, global_gain, in_proj, conv_weight, conv_bias, step_bias, decay_log, skip_gain, mixer_gain, out_proj, byte_table, local_gain, qkv_proj, attn_out, ffn_gain, gate_up, down_proj)))

    def one_sequence(totals, element):
        sequence, grad_out = element
        output, pullback = jax.vjp(lambda weights: layer(weights, sequence), params)
        gradients = pullback(grad_out.astype(jnp.float32))[0]
        return (tuple((summed + fresh for summed, fresh in zip(totals, gradients))), output.astype(jnp.bfloat16))
    starting = tuple((jnp.zeros(matrix.shape, jnp.float32) for matrix in params))
    totals, activations = lax.scan(one_sequence, starting, (byte_ids, cotangent))
    return (activations, totals[0], totals[1], totals[2], totals[3], totals[4], totals[5], totals[6], totals[7], totals[8], totals[9], totals[10], totals[11], totals[12], totals[13], totals[14], totals[15], totals[16])
```

```python
import functools

import jax
import jax.numpy as jnp
from jax import lax
from jax.experimental import pallas as pl
from jax.experimental.pallas import tpu as pltpu
from jax.sharding import PartitionSpec as P

D = 1024
NST = 128
HM = 32
HA = 16
FF = 4096
VOCAB = 256
KC = 4
PATCH = 8
DI = 2048
PM = 64
DA = 64
DG = 128
XBC = 2304
BC = XBC - DI
EPS = 1e-05
PAIRS = HA // 2
highest = lax.Precision.HIGHEST
bf16 = jnp.bfloat16
f32 = jnp.float32
VM = pl.BlockSpec(memory_space=pltpu.VMEM)


def grid_of(n):
    outer = max(n // 8, 1) if n >= 8 else 1
    return n // (2 * outer), outer


class Place:
    def __init__(self, n):
        self.n = n
        self.A, self.B = grid_of(n)
        me = lax.axis_index("fsdp")
        self.me = me
        self.c = me % 2
        self.b = (me // 2) % self.B
        self.a = me // (2 * self.B)

    def at(self, a, b, c):
        return (a * self.B + b) * 2 + c


def remote(src, dst, send, recv, peer):
    return pltpu.make_async_remote_copy(
        src_ref=src,
        dst_ref=dst,
        send_sem=send,
        recv_sem=recv,
        device_id={"fsdp": peer},
        device_id_type=pl.DeviceIdType.MESH,
    )


def gather_steps(pc, src, out, sems):
    send, recv = sems
    A, B = pc.A, pc.B
    started = []
    slot = [0]

    def push(block, where, peer):
        cp = remote(block, out.at[where], send.at[slot[0]], recv.at[where], peer)
        slot[0] += 1
        cp.start()
        started.append(cp)

    def arrived(where):
        remote(src, out.at[where], send.at[0], recv.at[where], pc.me).wait_recv()

    for off in range(1, A):
        push(src, pc.me, pc.at((pc.a + off) % A, pc.b, pc.c))
    for k in range(1, B):
        push(src, pc.me, pc.at(pc.a, (pc.b + k) % B, pc.c))
    push(src, pc.me, pc.at(pc.a, pc.b, 1 - pc.c))
    out[pc.me] = src[...]
    yield
    for off in range(1, A):
        where = pc.at((pc.a - off + A) % A, pc.b, pc.c)
        arrived(where)
        for k in range(1, B):
            push(out.at[where], where, pc.at(pc.a, (pc.b + k) % B, pc.c))
        push(out.at[where], where, pc.at(pc.a, pc.b, 1 - pc.c))
    yield
    for off in range(A):
        for k in range(1, B):
            where = pc.at((pc.a - off + A) % A, (pc.b - k + B) % B, pc.c)
            arrived(where)
            push(out.at[where], where, pc.at(pc.a, pc.b, 1 - pc.c))
    yield
    for a in range(A):
        for b in range(B):
            arrived(pc.at(a, b, 1 - pc.c))
    for cp in started:
        cp.wait_send()


def exchange_steps(pc, src, out, sems):
    send, recv = sems
    n = pc.n
    started = []
    for k in range(1, n):
        peer = (pc.me + k) % n
        cp = remote(src.at[peer], out.at[pc.me], send.at[k - 1], recv.at[pc.me], peer)
        cp.start()
        started.append(cp)
    out[pc.me] = src[pc.me]
    yield
    yield
    yield
    for k in range(1, n):
        peer = (pc.me + k) % n
        remote(src.at[peer], out.at[peer], send.at[k - 1], recv.at[peer], pc.me).wait_recv()
    for cp in started:
        cp.wait_send()


def sum_steps(pc, src, out, scratch):
    r1, s1, r2, s2, r3, send1, recv1, send2, recv2, send3, recv3 = scratch
    A, B = pc.A, pc.B
    started = []
    order = [(pc.a + off) % A for off in list(range(1, A)) + [0]]

    def begin(cp):
        cp.start()
        started.append(cp)

    def copy1(a):
        return remote(
            src.at[a, :, 1 - pc.c], r1.at[a], send1.at[a], recv1.at[a], pc.at(pc.a, pc.b, 1 - pc.c)
        )

    def copy2(a, k):
        to = (pc.b + k) % B
        return remote(
            s1.at[a, to], r2.at[a, k - 1], send2.at[a, k - 1], recv2.at[a, k - 1],
            pc.at(pc.a, to, pc.c),
        )

    def copy3(a, off):
        return remote(
            s2.at[a], r3.at[off - 1], send3.at[off - 1], recv3.at[off - 1], pc.at(a, pc.b, pc.c)
        )

    for a in order:
        begin(copy1(a))
    yield
    for a in order:
        copy1(a).wait_recv()
        for k in range(1, B):
            to = (pc.b + k) % B
            s1[a, to] = (src[a, to, pc.c].astype(f32) + r1[a, to].astype(f32)).astype(s1.dtype)
            begin(copy2(a, k))
    yield
    for off, a in zip(list(range(1, A)) + [0], order):
        total = src[a, pc.b, pc.c].astype(f32) + r1[a, pc.b].astype(f32)
        for k in range(1, B):
            copy2(a, k).wait_recv()
            total = total + r2[a, k - 1].astype(f32)
        if off > 0:
            s2[a] = total.astype(s2.dtype)
            begin(copy3(a, off))
        else:
            out[...] = total
    yield
    for off in range(1, A):
        copy3(pc.a, off).wait_recv()
        out[...] += r3[off - 1].astype(f32)
    for cp in started:
        cp.wait_send()


def scratch_of(kind, x, n):
    A, B = grid_of(n)
    dma = pltpu.SemaphoreType.DMA
    if kind == "gather":
        return [dma((2 * n,)), dma((n,))]
    if kind == "exchange":
        return [dma((n,)), dma((n,))]
    r, c = x.shape[-2:]
    return [
        pltpu.VMEM((A, B, r, c), x.dtype),
        pltpu.VMEM((A, B, r, c), x.dtype),
        pltpu.VMEM((A, max(B - 1, 1), r, c), x.dtype),
        pltpu.VMEM((A, r, c), x.dtype),
        pltpu.VMEM((max(A - 1, 1), r, c), x.dtype),
        dma((A,)),
        dma((A,)),
        dma((A, max(B - 1, 1))),
        dma((A, max(B - 1, 1))),
        dma((max(A - 1, 1),)),
        dma((max(A - 1, 1),)),
    ]


STEPS = {"gather": gather_steps, "exchange": exchange_steps, "sum": sum_steps}


def comm_kernel(kinds, counts, n, *refs):
    m = len(kinds)
    ins, outs, rest = refs[:m], refs[m : 2 * m], refs[2 * m :]
    pc = Place(n)
    barrier = pltpu.get_barrier_semaphore()
    if "exchange" in kinds:
        peers = [(pc.me + k) % n for k in range(1, n)]
    else:
        peers = [pc.at((pc.a + k) % pc.A, pc.b, pc.c) for k in range(1, pc.A)]
        peers += [pc.at(pc.a, (pc.b + k) % pc.B, pc.c) for k in range(1, pc.B)]
        peers += [pc.at(pc.a, pc.b, 1 - pc.c)]
    for peer in peers:
        pl.semaphore_signal(
            barrier, inc=1, device_id={"fsdp": peer}, device_id_type=pl.DeviceIdType.MESH
        )
    pl.semaphore_wait(barrier, len(peers))
    live = []
    for kind, count, src, out in zip(kinds, counts, ins, outs):
        live.append(STEPS[kind](pc, src, out, rest[:count]))
        rest = rest[count:]
    while live:
        left = []
        for steps in live:
            try:
                next(steps)
                left.append(steps)
            except StopIteration:
                pass
        live = left


def communicate(n, cid, *jobs):
    A, B = grid_of(n)
    kinds, ins, outs, scratch, counts = [], [], [], [], []
    for kind, x in jobs:
        kinds.append(kind)
        if kind == "gather":
            outs.append(jax.ShapeDtypeStruct((n,) + x.shape, x.dtype))
        elif kind == "exchange":
            outs.append(jax.ShapeDtypeStruct(x.shape, x.dtype))
        else:
            outs.append(jax.ShapeDtypeStruct(x.shape[-2:], f32))
        own = scratch_of(kind, x, n)
        counts.append(len(own))
        scratch += own
        ins.append(x.reshape((A, B, 2) + x.shape[1:]) if kind == "sum" else x)
    return pl.pallas_call(
        functools.partial(comm_kernel, tuple(kinds), tuple(counts), n),
        out_shape=tuple(outs),
        in_specs=[VM] * len(ins),
        out_specs=tuple([VM] * len(ins)),
        scratch_shapes=scratch,
        compiler_params=pltpu.CompilerParams(
            collective_id=cid, has_side_effects=True, vmem_limit_bytes=60 * 1024 * 1024
        ),
        name="comm_%d" % cid,
    )(*ins)


def rms_back(dy, v, gain, r):
    dyg = dy * gain
    m = jnp.mean(dyg * v, axis=-1, keepdims=True)
    return r * dyg - v * (r * r * r) * m, jnp.sum(dy * v * r, axis=0)


def row_scale(v):
    return lax.rsqrt(jnp.mean(v * v, axis=-1, keepdims=True) + EPS)


def dot(a, b, dims=((1,), (0,))):
    return lax.dot_general(a, b, (dims, ((), ())), preferred_element_type=f32)


NT = ((1,), (1,))
TN = ((0,), (0,))


def head_parts(rows):
    lane = lax.broadcasted_iota(jnp.int32, (rows, 2 * DA), 1)
    ri = lax.broadcasted_iota(jnp.int32, (rows, rows), 0)
    ci = lax.broadcasted_iota(jnp.int32, (rows, rows), 1)
    allowed = jnp.logical_and(ri // PATCH == ci // PATCH, ci <= ri)
    return (lane < DA, lane >= DA), allowed


def weights_of(q, k, allowed):
    s = dot(q, k, NT) * (DA**-0.5)
    s = jnp.where(allowed, s, -1e30)
    e = jnp.exp(s - jnp.max(s, axis=-1, keepdims=True))
    return e / jnp.sum(e, axis=-1, keepdims=True)


def attend_kernel(qkv_ref, out_ref):
    rows = qkv_ref.shape[0]
    sides, allowed = head_parts(rows)
    for pair in range(PAIRS):
        lo = pair * 2 * DA
        q = qkv_ref[:, lo : lo + 2 * DA].astype(bf16)
        k = qkv_ref[:, D + lo : D + lo + 2 * DA].astype(bf16)
        v = qkv_ref[:, 2 * D + lo : 2 * D + lo + 2 * DA].astype(bf16)
        parts = []
        for side in sides:
            p = weights_of(jnp.where(side, q, jnp.zeros_like(q)), k, allowed)
            parts.append(dot(p.astype(bf16), v))
        out_ref[:, lo : lo + 2 * DA] = jnp.where(sides[0], parts[0], parts[1]).astype(bf16)


def attend(qkv):
    return pl.pallas_call(
        attend_kernel,
        out_shape=jax.ShapeDtypeStruct((qkv.shape[0], D), bf16),
        in_specs=[VM],
        out_specs=VM,
        name="attend",
    )(qkv)


def attend_back_kernel(qkv_ref, g_ref, out_ref):
    rows = qkv_ref.shape[0]
    sides, allowed = head_parts(rows)
    scale = DA**-0.5
    for pair in range(PAIRS):
        lo = pair * 2 * DA
        q = qkv_ref[:, lo : lo + 2 * DA].astype(bf16)
        k = qkv_ref[:, D + lo : D + lo + 2 * DA].astype(bf16)
        v = qkv_ref[:, 2 * D + lo : 2 * D + lo + 2 * DA].astype(bf16)
        g = g_ref[:, lo : lo + 2 * DA].astype(bf16)
        dq, dk, dv = [], [], []
        for side in sides:
            p = weights_of(jnp.where(side, q, jnp.zeros_like(q)), k, allowed)
            dp = dot(jnp.where(side, g, jnp.zeros_like(g)), v, NT)
            ds = p * (dp - jnp.sum(dp * p, axis=-1, keepdims=True))
            ds = ds.astype(bf16)
            dq.append(dot(ds, k) * scale)
            dk.append(dot(ds, q, TN) * scale)
            dv.append(dot(p.astype(bf16), g, TN))
        for j, parts in enumerate((dq, dk, dv)):
            out_ref[:, j * D + lo : j * D + lo + 2 * DA] = jnp.where(
                sides[0], parts[0], parts[1]
            ).astype(bf16)


def attend_back(qkv, g):
    return pl.pallas_call(
        attend_back_kernel,
        out_shape=jax.ShapeDtypeStruct(qkv.shape, bf16),
        in_specs=[VM, VM],
        out_specs=VM,
        name="attend_back",
    )(qkv, g)


def mixer(conv_in, taps, bias, step_raw, step_bias, decay_log, skip, gate, width):
    length = conv_in.shape[0]
    heads = width // PM
    padded = jnp.concatenate([jnp.zeros((KC - 1, conv_in.shape[1]), f32), conv_in], 0)
    summed = bias
    for k in range(KC):
        summed = summed + padded[k : k + length] * taps[k]
    out = jax.nn.silu(summed)
    x, b, c = out[:, :width], out[:, width : width + NST], out[:, width + NST :]
    step = jax.nn.softplus(step_raw + step_bias)
    ri = lax.broadcasted_iota(jnp.int32, (length, length), 0)
    ci = lax.broadcasted_iota(jnp.int32, (length, length), 1)
    causal = ci <= ri
    logs = step * -jnp.exp(decay_log)
    total = jnp.dot(causal.astype(f32), logs, precision=highest).T
    spread = total[:, :, None] - total[:, None, :]
    decay = jnp.exp(jnp.where(causal[None], spread, -jnp.inf))
    cb = lax.dot_general(c, b, (NT, ((), ())), precision=highest)
    xh = x.reshape(length, heads, PM)
    scaled = xh * step[..., None]
    joined = jnp.einsum("htu,uhp->thp", cb[None] * decay, scaled, precision=highest)
    joined = joined + skip[:, None] * xh
    return joined.reshape(length, width) * jax.nn.silu(gate)


def across(x, dp):
    if dp == 1:
        return x.astype(f32)
    if dp > 2:
        return lax.psum(x, "dp").astype(f32)
    x = lax.optimization_barrier(x)
    return x.astype(f32) + lax.ppermute(x, "dp", [(0, 1), (1, 0)]).astype(f32)


def on_device(
    n,
    dp,
    byte_ids,
    cotangent,
    patch_table,
    global_gain,
    in_proj,
    conv_weight,
    conv_bias,
    step_bias,
    decay_log,
    skip_gain,
    mixer_gain,
    out_proj,
    byte_table,
    local_gain,
    qkv_proj,
    attn_out,
    ffn_gain,
    gate_up,
    down_proj,
):
    me = lax.axis_index("fsdp")
    _, L = byte_ids.shape
    own_p = L // PATCH
    T = own_p * n
    R = L * n
    dn, fn, wn, hn = D // n, FF // n, DI // n, HM // n
    xn = XBC // n
    ids = byte_ids.reshape(L)

    gather = functools.partial(lax.all_gather, axis_name="fsdp", axis=0, tiled=True)
    qkv_full = gather(qkv_proj)
    byte_full = gather(byte_table)
    attn_full = gather(attn_out)
    cot_all = gather(cotangent.reshape(L, D))

    zx = in_proj[:, : 2 * DI].reshape(dn, 2, n, wn).transpose(2, 0, 1, 3).reshape(n, dn, 2 * wn)
    shared = jnp.pad(in_proj[:, 2 * DI :], ((0, 0), (0, 384 - (BC + HM))))
    gu = gate_up.reshape(dn, 2, n, fn).transpose(2, 0, 1, 3).reshape(n, dn, 2 * fn)
    vectors = [global_gain, local_gain, ffn_gain, conv_weight.reshape(-1), conv_bias,
               step_bias, decay_log, skip_gain]
    sizes = [v.shape[0] for v in vectors]
    packed = jnp.concatenate(vectors)
    packed = jnp.pad(packed, (0, 2048 - packed.shape[0])).reshape(16, 128)
    ids_all, small, table, shared_w, zx_w, gu_w = communicate(
        n, 0,
        ("gather", ids.reshape(1, L)),
        ("gather", packed),
        ("gather", patch_table),
        ("gather", shared),
        ("exchange", zx),
        ("exchange", gu),
    )
    small = small.reshape(n, 2048).astype(f32)
    full = []
    at = 0
    for s in sizes:
        full.append(small[:, at : at + s].reshape(-1))
        at += s
    g_gain, l_gain, f_gain, taps_all, bias_all = full[:5]
    taps_all = taps_all.reshape(XBC, KC)
    taps = jnp.concatenate(
        [lax.dynamic_slice_in_dim(taps_all, me * wn, wn, 0), taps_all[DI:]], 0
    ).T
    bias = jnp.concatenate([lax.dynamic_slice_in_dim(bias_all, me * wn, wn, 0), bias_all[DI:]], 0)
    w_mix = jnp.concatenate([zx_w.reshape(D, 2 * wn), shared_w.reshape(D, 384)], 1)
    w_gu = gu_w.reshape(D, 2 * fn)
    table = table.reshape(PATCH, VOCAB, DG)

    grid = ids_all.reshape(T, PATCH)
    earlier = jnp.concatenate([jnp.full((1, PATCH), -1, jnp.int32), grid[:-1]], 0)
    hot = (earlier[..., None] == jnp.arange(VOCAB, dtype=jnp.int32)).astype(bf16)
    patch_input = jnp.einsum("pjv,jvc->pjc", hot, table, preferred_element_type=f32).reshape(T, D)
    r_g = row_scale(patch_input)
    normed = (patch_input * r_g * g_gain).astype(bf16)
    proj = dot(normed, w_mix)
    gate_z = proj[:, :wn]
    conv_in = proj[:, wn : 2 * wn + BC]
    dt_all = proj[:, 2 * wn + BC : 2 * wn + BC + HM]
    dt_raw = lax.dynamic_slice_in_dim(dt_all, me * hn, hn, 1)
    y, pull_mixer = jax.vjp(
        functools.partial(mixer, width=wn),
        conv_in, taps, bias, dt_raw, step_bias.astype(f32), decay_log.astype(f32),
        skip_gain.astype(f32), gate_z,
    )
    m_gain = mixer_gain.astype(f32)
    part = dot((y * m_gain).astype(bf16), out_proj)
    squares = jnp.broadcast_to(jnp.sum(y * y, axis=-1, keepdims=True), (T, 128))
    payload = jnp.concatenate([part, squares], 1).astype(bf16).reshape(n, own_p, D + 128)
    (summed,) = communicate(n, 1, ("sum", payload))
    out_sum = summed[:, :D]
    r_m = lax.rsqrt(summed[:, D : D + 1] * (1.0 / DI) + EPS)
    own_input = lax.dynamic_slice_in_dim(patch_input, me * own_p, own_p, 0)
    own_r_g = lax.dynamic_slice_in_dim(r_g, me * own_p, own_p, 0)
    patch_out = own_input + r_m * out_sum

    byte_hot = (ids[:, None] == jnp.arange(VOCAB, dtype=jnp.int32)[None, :]).astype(bf16)
    spread = jnp.broadcast_to(patch_out[:, None, :], (own_p, PATCH, D)).reshape(L, D)
    stream = dot(byte_hot, byte_full) + spread
    r_l = row_scale(stream)
    first_norm = (stream * r_l * l_gain).astype(bf16)
    qkv = dot(first_norm, qkv_full)
    attended = attend(qkv)
    residual = stream + dot(attended, attn_full)
    r_f = row_scale(residual)
    second_norm = (residual * r_f * f_gain).astype(bf16)

    (x_all,) = communicate(n, 2, ("gather", second_norm))
    x_all = x_all.reshape(R, D)
    gates = dot(x_all, w_gu)
    gate, up = gates[:, :fn], gates[:, fn:]
    sig = jax.nn.sigmoid(gate)
    act = gate * sig
    hidden = (act * up).astype(bf16)
    y_part = dot(hidden, down_proj)
    g_hidden = dot(cot_all, down_proj, NT)
    d_gate = g_hidden * up * (sig * (1.0 + gate * (1.0 - sig)))
    grad_gates = jnp.concatenate([d_gate, g_hidden * act], 1).astype(bf16)
    gs_part = dot(grad_gates, w_gu, NT)
    both = jnp.concatenate([y_part, gs_part], 1).astype(bf16).reshape(n, L, 2 * D)
    (both,) = communicate(n, 3, ("sum", both))
    activations = (residual + both[:, :D]).astype(bf16).reshape(1, L, D)
    grad_second = both[:, D:]
    grad_down = dot(hidden, cot_all, TN).astype(bf16)
    grad_gu = dot(x_all, grad_gates, TN).astype(bf16).reshape(n, dn, 2 * fn)
    down_out = across(grad_down, dp)

    res_norm, d_f_gain = rms_back(grad_second, residual, f_gain, r_f)
    grad_residual = cotangent.reshape(L, D).astype(f32) + res_norm
    res_low = grad_residual.astype(bf16)
    scatter = functools.partial(
        lax.psum_scatter, axis_name="fsdp", scatter_dimension=0, tiled=True
    )
    attn_g = scatter(dot(attended, res_low, TN).astype(bf16))
    g_att = dot(res_low, attn_full, NT)
    grad_qkv_rows = attend_back(qkv, g_att)
    qkv_g = scatter(dot(first_norm, grad_qkv_rows, TN).astype(bf16))
    grad_first = dot(grad_qkv_rows, qkv_full, NT)
    stream_norm, d_l_gain = rms_back(grad_first, stream, l_gain, r_l)
    grad_stream = grad_residual + stream_norm
    byte_g = scatter(dot(byte_hot, grad_stream.astype(bf16), TN).astype(bf16))
    gpo_own = grad_stream.reshape(own_p, PATCH, D).sum(axis=1)
    gpo_low = gpo_own.astype(bf16)
    mean_own = jnp.sum(gpo_low.astype(f32) * out_sum, axis=-1, keepdims=True) * (1.0 / DI)
    lane = lax.broadcasted_iota(jnp.int32, (own_p, 128), 1)
    scal = jnp.where(lane == 0, r_m, mean_own)
    gpo, scal, gu_back = communicate(
        n, 4, ("gather", gpo_low), ("gather", scal), ("exchange", grad_gu)
    )
    gpo = gpo.reshape(T, D)
    scal = scal.reshape(T, 128)
    r_m_all, mean_all = scal[:, 0:1], scal[:, 1:2]
    gu_rows = gu_back.reshape(n, dn, 2, fn).transpose(1, 2, 0, 3).reshape(dn, 2 * FF)
    gu_out = across(gu_rows, dp)

    mixer_low = (y * r_m_all * m_gain).astype(bf16)
    op_out = across(dot(mixer_low, gpo, TN).astype(bf16), dp)
    g_mix = dot(gpo, out_proj, NT)
    d_m_gain = jnp.sum(g_mix * y * r_m_all, axis=0)
    grad_y = r_m_all * (g_mix * m_gain) - y * (r_m_all * r_m_all * r_m_all) * mean_all
    d_conv, d_taps, d_bias, d_dt, d_step_b, d_decay, d_skip, d_z = pull_mixer(grad_y)
    dt_cols = lax.dynamic_update_slice(jnp.zeros((T, 384 - BC), f32), d_dt, (0, me * hn))
    gp = jnp.concatenate([d_z, d_conv, dt_cols], 1).astype(bf16)
    gn_part = dot(gp, w_mix, NT).astype(bf16).reshape(n, own_p, D)
    g_w = dot(normed, gp, TN).astype(bf16).reshape(n, dn, 2 * wn + 384)
    zx_g, sh_g, gn = communicate(
        n, 5, ("exchange", g_w[:, :, : 2 * wn]), ("sum", g_w[:, :, 2 * wn :]), ("sum", gn_part)
    )
    zx_rows = zx_g.reshape(n, dn, 2, wn).transpose(1, 2, 0, 3).reshape(dn, 2 * DI)
    in_rows = jnp.concatenate([zx_rows, sh_g[:, : BC + HM].astype(bf16)], 1)
    in_out = across(in_rows, dp)
    d_in, d_g_gain = rms_back(gn, own_input, g_gain, own_r_g)
    gil = (d_in + gpo_own).astype(bf16)

    taps_grad = jnp.zeros((XBC, KC), f32)
    taps_grad = lax.dynamic_update_slice(taps_grad, d_taps[:, :wn].T, (me * wn, 0))
    taps_grad = lax.dynamic_update_slice(taps_grad, d_taps[:, wn:].T, (DI, 0))
    bias_grad = jnp.zeros((XBC,), f32)
    bias_grad = lax.dynamic_update_slice(bias_grad, d_bias[:wn], (me * wn,))
    bias_grad = lax.dynamic_update_slice(bias_grad, d_bias[wn:], (DI,))
    terms = jnp.concatenate(
        [d_g_gain.reshape(n, dn), d_l_gain.reshape(n, dn), d_f_gain.reshape(n, dn),
         taps_grad.reshape(n, xn * KC), bias_grad.reshape(n, xn)], 1
    )
    terms = jnp.pad(terms, ((0, 0), (0, 1024 - terms.shape[1]))).reshape(n, 8, 128)
    gil_all, own_terms = communicate(n, 6, ("gather", gil), ("sum", terms))
    gil_all = gil_all.reshape(T, D)
    rows_n = PATCH * VOCAB // n
    j = (me * rows_n) // VOCAB
    first_row = (me * rows_n) % VOCAB
    own_ids = lax.dynamic_slice_in_dim(earlier, j, 1, 1)
    own_hot = (own_ids == first_row + jnp.arange(rows_n, dtype=jnp.int32)[None, :]).astype(bf16)
    pt_own = dot(own_hot, lax.dynamic_slice_in_dim(gil_all, j * DG, DG, 1), TN)
    rest = jnp.concatenate([own_terms.reshape(-1), d_m_gain, d_step_b, d_decay, d_skip])
    pt_out = across(pt_own, dp)
    rest = across(rest, dp)
    cut = [dn, dn, dn, xn * KC, xn, 1024 - 3 * dn - xn * (KC + 1), wn, hn, hn, hn]
    bits = []
    at = 0
    for s in cut:
        bits.append(rest[at : at + s])
        at += s
    return (
        activations,
        pt_out,
        bits[0],
        in_out,
        bits[3].reshape(xn, KC),
        bits[4],
        bits[7],
        bits[8],
        bits[9],
        bits[6],
        op_out,
        across(byte_g, dp),
        bits[1],
        across(qkv_g, dp),
        across(attn_g, dp),
        bits[2],
        gu_out,
        down_out,
    )


def solution(mesh):
    row, mat = P("fsdp"), P("fsdp", None)
    in_specs = (
        P("dp", "fsdp"), P("dp", "fsdp", None), mat, row, mat, mat, row, row, row, row, row,
        mat, mat, row, mat, mat, row, mat, mat,
    )
    out_specs = (
        P("dp", "fsdp", None), mat, row, mat, mat, row, row, row, row, row, mat, mat, row,
        mat, mat, row, mat, mat,
    )
    body = functools.partial(on_device, mesh.shape["fsdp"], mesh.shape["dp"])
    return jax.shard_map(body, mesh=mesh, in_specs=in_specs, out_specs=out_specs, check_vma=False)
```
